16 devices in a mesh: rep: 1, dp: 16 (over x, y, z, core).
Axes of the slice: x: 2, y: 2, z: 2, core: 2. Of those that a mesh axis runs over, the one named last changes fastest.
Arguments:
- a: bfloat16 [16, 4, 4096, 1280], P(('rep', 'dp'))
- g: bfloat16 [16, 4, 4096, 3072], P(('rep', 'dp'))
Outputs:
- output: bfloat16 [4, 1280, 3072], P('rep')
All inputs are finite; a program needn't handle non-finite values.
Results may differ from the reference program's by a relative error of at most 0.012.
Values are sent between devices in bfloat16 or wider.
A program may use at most 2 GiB of HBM per device.

```python
import jax
import jax.numpy as jnp
from jax import lax

DEVICES = 16
MATRICES = 4
TOKENS = 4096
D = 1280
FF = 3072


def setup_inputs(seed: int = 0, part: int = 0) -> dict:
    ka, kg, ks = (jax.random.fold_in(k, part) for k in jax.random.split(jax.random.key(seed), 3))
    size = 2.0 ** jax.random.uniform(ks, (DEVICES, MATRICES, 1, 1), jnp.float32, -1.0, 1.0)
    a = jax.random.normal(ka, (DEVICES, MATRICES, TOKENS, D), jnp.float32)
    g = size * jax.random.normal(kg, (DEVICES, MATRICES, TOKENS, FF), jnp.float32) * (DEVICES * TOKENS) ** -0.5
    return {"a": a.astype(jnp.bfloat16), "g": g.astype(jnp.bfloat16)}


def reference(a, g):
    def take(so_far, one):
        return so_far + jnp.einsum("ntd,ntf->ndf", *one, preferred_element_type=jnp.float32), None

    return lax.scan(take, jnp.zeros((MATRICES, D, FF), jnp.float32), (a, g))[0].astype(jnp.bfloat16)
```

```python
import functools

import jax
import jax.numpy as jnp
from jax import lax
from jax.experimental import pallas as pl
from jax.experimental.pallas import tpu as pltpu
from jax.sharding import PartitionSpec as P

COLS = 256
CHUNK = 512
LAG = 3


def kernel(a_ref, g_ref, out_ref, at, gb, stg, own, ag, s0s, r1s, r2s, r3s, r1r, r2r, r3r,
           s0_send, s0_recv, r1_send, r1_recv, r2_send, r2_recv, r3_send, r3_recv,
           ag1_recv, ag2_recv, ag3_recv, ag1_send, ag2_send, ag3_send, core_send, core_recv, out_sem, g_sem, a_sem):
    _, mats, tokens, d = a_ref.shape
    per = g_ref.shape[3] // COLS
    units = mats * per
    chunks = tokens // CHUNK
    half, q1, q2, q3 = d // 2, d // 4, d // 8, d // 16
    f32, bf16 = jnp.float32, jnp.bfloat16

    me = lax.axis_index("dp")
    bit = {k: lax.rem(me // k, 2) for k in (8, 4, 2, 1)}
    peer = {k: me + k - 2 * k * bit[k] for k in (8, 4, 2, 1)}
    c = bit[1]

    barrier = pltpu.get_barrier_semaphore()
    for k in (8, 4, 2, 1):
        pl.semaphore_signal(barrier, inc=1, device_id={"dp": peer[k]}, device_id_type=pl.DeviceIdType.MESH)
    pl.semaphore_wait(barrier, 4)

    def dims(w):
        r = lax.rem(w, 3)

        def sel(x, y, z):
            return jnp.where(r == 0, x, jnp.where(r == 1, y, z))

        b = (sel(bit[8], bit[4], bit[2]), sel(bit[4], bit[2], bit[8]), sel(bit[2], bit[8], bit[4]))
        p = (sel(peer[8], peer[4], peer[2]), sel(peer[4], peer[2], peer[8]), sel(peer[2], peer[8], peer[4]))
        return b, p

    def rows(start, size):
        return pl.ds(pl.multiple_of(start, 16), size)

    def remote(src, dst, send, recv, to):
        return pltpu.make_async_remote_copy(src_ref=src, dst_ref=dst, send_sem=send, recv_sem=recv,
                                            device_id={"dp": to}, device_id_type=pl.DeviceIdType.MESH)

    def load_g(t):
        n, j = t // per, lax.rem(t, per)
        slot = lax.rem(t, 2)
        return pltpu.make_async_copy(
            g_ref.at[0, n, :, pl.ds(pl.multiple_of(j * COLS, COLS), COLS)], gb.at[slot], g_sem.at[slot])

    def load_a(n, i):
        slot = lax.rem(i, 2)
        return pltpu.make_async_copy(
            a_ref.at[0, n, pl.ds(pl.multiple_of(i * CHUNK, CHUNK), CHUNK), :], stg.at[slot], a_sem.at[slot])

    def transpose(n, i):
        at[lax.rem(n, 2), :, pl.ds(pl.multiple_of(i * CHUNK, CHUNK), CHUNK)] = stg[lax.rem(i, 2)].T

    def dot(t, row):
        return jnp.dot(at[lax.rem(t // per, 2), rows(row, half), :], gb[lax.rem(t, 2)], preferred_element_type=f32)

    def s0(w):
        k = lax.rem(w, 3)
        return remote(s0s.at[k], ag.at[w], s0_send.at[k], s0_recv.at[lax.rem(w, 4)], peer[1])

    def r1(w):
        k, m = lax.rem(w, 4), lax.rem(w, 6)
        return remote(r1s.at[k], r1r.at[m], r1_send.at[k], r1_recv.at[m], dims(w)[1][0])

    def r2(w):
        k, m = lax.rem(w, 4), lax.rem(w, 6)
        return remote(r2s.at[k], r2r.at[m], r2_send.at[k], r2_recv.at[m], dims(w)[1][1])

    def r3(w):
        k, m = lax.rem(w, 4), lax.rem(w, 6)
        return remote(r3s.at[k], r3r.at[m], r3_send.at[k], r3_recv.at[m], dims(w)[1][2])

    def g1(v):
        b, p = dims(v)
        part = ag.at[v, rows(b[0] * q1 + b[1] * q2 + b[2] * q3, q3)]
        return remote(part, part, ag1_send, ag1_recv.at[v], p[2])

    def g2(v):
        b, p = dims(v)
        part = ag.at[v, rows(b[0] * q1 + b[1] * q2, q2)]
        return remote(part, part, ag2_send, ag2_recv.at[v], p[1])

    def g3(v):
        b, p = dims(v)
        part = ag.at[v, rows(b[0] * q1, q1)]
        return remote(part, part, ag3_send, ag3_recv.at[v], p[0])

    def target(v):
        return out_ref.at[v // per, rows(c * half, half), pl.ds(pl.multiple_of(lax.rem(v, per) * COLS, COLS), COLS)]

    def finish(v):
        remote(ag.at[v], target(v), core_send, core_recv, peer[1]).start()
        pltpu.make_async_copy(ag.at[v], target(v), out_sem).start()

    def add1(w):
        k = lax.rem(w, 8)
        (b1, _, _), _ = dims(w)
        give, keep = rows((1 - b1) * q1, q1), rows(b1 * q1, q1)
        r1s[lax.rem(w, 4)] = (own[k, give] + ag[w, give].astype(f32)).astype(bf16)
        own[k, keep] = own[k, keep] + ag[w, keep].astype(f32)

    def add2(w):
        k, m = lax.rem(w, 8), lax.rem(w, 6)
        (b1, b2, _), _ = dims(w)
        give, keep = (1 - b2) * q2, b2 * q2
        r2s[lax.rem(w, 4)] = (own[k, rows(b1 * q1 + give, q2)] + r1r[m, rows(give, q2)].astype(f32)).astype(bf16)
        kept = rows(b1 * q1 + keep, q2)
        own[k, kept] = own[k, kept] + r1r[m, rows(keep, q2)].astype(f32)

    def add3(w):
        k, m = lax.rem(w, 8), lax.rem(w, 6)
        (b1, b2, b3), _ = dims(w)
        base = b1 * q1 + b2 * q2
        give, keep = (1 - b3) * q3, b3 * q3
        r3s[lax.rem(w, 4)] = (own[k, rows(base + give, q3)] + r2r[m, rows(give, q3)].astype(f32)).astype(bf16)
        kept = rows(base + keep, q3)
        own[k, kept] = own[k, kept] + r2r[m, rows(keep, q3)].astype(f32)

    def add4(w):
        k, m = lax.rem(w, 8), lax.rem(w, 6)
        (b1, b2, b3), _ = dims(w)
        kept = rows(b1 * q1 + b2 * q2 + b3 * q3, q3)
        ag[w, kept] = (own[k, kept] + r3r[m].astype(f32)).astype(bf16)

    def step(t, compute, guard):
        def when(cond, f):
            if guard:
                pl.when(cond)(f)
            else:
                f()

        def live(lag):
            return jnp.logical_and(t >= lag, t - lag < units)

        if compute:
            n, j = t // per, lax.rem(t, per)
            more = n + 1 < mats

            @pl.when(t + 1 < units)
            def _():
                load_g(t + 1).start()

            @pl.when(jnp.logical_and(more, j == 0))
            def _():
                load_a(n + 1, 0).start()

            @pl.when(jnp.logical_and(more, j + 1 < chunks))
            def _():
                load_a(n + 1, j + 1).start()

            @pl.when(jnp.logical_and(more, j < chunks))
            def _():
                load_a(n + 1, j).wait()
                transpose(n + 1, j)

            when(t >= 3, lambda: s0(t - 3).wait_send())
            load_g(t).wait()
            s0s[lax.rem(t, 3)] = dot(t, (1 - c) * half).astype(bf16)
            s0(t).start()

        def waits1():
            s0(t - 1).wait_recv()

        when(live(1), waits1)
        when(live(5), lambda: r1(t - 5).wait_send())
        when(live(3), lambda: r1(t - 3).wait_recv())
        when(live(7), lambda: r2(t - 7).wait_send())
        when(live(5), lambda: r2(t - 5).wait_recv())
        when(live(9), lambda: r3(t - 9).wait_send())
        when(live(7), lambda: r3(t - 7).wait_recv())
        when(live(1), lambda: add1(t - 1))
        when(live(3), lambda: add2(t - 3))
        when(live(5), lambda: add3(t - 5))
        when(live(7), lambda: add4(t - 7))
        if compute:
            own[lax.rem(t, 8)] = dot(t, c * half)
        when(live(1), lambda: r1(t - 1).start())
        when(live(3), lambda: r2(t - 3).start())
        when(live(5), lambda: r3(t - 5).start())

        def gather2():
            g1(t - 9 - LAG).wait_recv()
            g2(t - 9 - LAG).start()

        def gather3():
            g2(t - 9 - 2 * LAG).wait_recv()
            g3(t - 9 - 2 * LAG).start()

        def gather4():
            g3(t - 9 - 3 * LAG).wait_recv()
            finish(t - 9 - 3 * LAG)

        when(live(9), lambda: g1(t - 9).start())
        when(live(9 + LAG), gather2)
        when(live(9 + 2 * LAG), gather3)
        when(live(9 + 3 * LAG), gather4)

    def loop(lo, hi, compute, guard):
        def body(t, _):
            step(t, compute, guard)
            return 0

        lax.fori_loop(lo, hi, body, 0)

    load_g(0).start()
    load_a(0, 0).start()

    def first(i, _):
        @pl.when(i + 1 < chunks)
        def _():
            load_a(0, i + 1).start()

        load_a(0, i).wait()
        transpose(0, i)
        return 0

    lax.fori_loop(0, chunks, first, 0)

    deep = 9 + 3 * LAG
    loop(0, deep, True, True)
    loop(deep, units, True, False)
    loop(units, units + deep, False, True)

    for k in range(units - 3, units):
        s0(k).wait_send()

    def all_of(size, sem):
        whole = ag.at[pl.ds(0, units * size // half)]
        pltpu.make_async_copy(whole, whole, sem).wait()

    all_of(q3, ag1_send)
    all_of(q2, ag2_send)
    all_of(q1, ag3_send)
    all_of(half, core_send)
    all_of(half, core_recv)
    all_of(half, out_sem)


def solution(mesh):
    def step(a, g):
        _, mats, tokens, d = a.shape
        ff = g.shape[3]
        units = mats * ff // COLS
        half = d // 2
        bf16 = jnp.bfloat16
        dma = pltpu.SemaphoreType.DMA
        return pl.pallas_call(
            kernel,
            out_shape=jax.ShapeDtypeStruct((mats, d, ff), bf16),
            in_specs=[pl.BlockSpec(memory_space=pl.ANY)] * 2,
            out_specs=pl.BlockSpec(memory_space=pl.ANY),
            scratch_shapes=[
                pltpu.VMEM((2, d, tokens), bf16),
                pltpu.VMEM((2, tokens, COLS), bf16),
                pltpu.VMEM((2, CHUNK, d), bf16),
                pltpu.VMEM((8, half, COLS), jnp.float32),
                pltpu.VMEM((units, half, COLS), bf16),
                pltpu.VMEM((3, half, COLS), bf16),
                pltpu.VMEM((4, half // 2, COLS), bf16),
                pltpu.VMEM((4, half // 4, COLS), bf16),
                pltpu.VMEM((4, half // 8, COLS), bf16),
                pltpu.VMEM((6, half // 2, COLS), bf16),
                pltpu.VMEM((6, half // 4, COLS), bf16),
                pltpu.VMEM((6, half // 8, COLS), bf16),
                dma((3,)), dma((4,)), dma((4,)), dma((6,)), dma((4,)), dma((6,)), dma((4,)), dma((6,)),
                dma((units,)), dma((units,)), dma((units,)), dma, dma, dma, dma, dma, dma, dma((2,)), dma((2,)),
            ],
            compiler_params=pltpu.CompilerParams(
                collective_id=0, has_side_effects=True, vmem_limit_bytes=64 * 1024 * 1024 - 65536),
            name="grads",
        )(a, g)

    return jax.shard_map(step, mesh=mesh, in_specs=(P(("rep", "dp")),) * 2, out_specs=P("rep"), check_vma=False)
```

```python
import functools

import jax
import jax.numpy as jnp
from jax import lax
from jax.experimental import pallas as pl
from jax.experimental.pallas import tpu as pltpu
from jax.sharding import PartitionSpec as P

COLS = 256
CHUNK = 512
LAG = 3
E1, E2, E3, E4, G1 = 1, 3, 5, 6, 6
TURN = 3
RING = 6
LAND = 12
PIECE = 80
HELD = 12
ORDERS = ((8, 4, 2), (4, 2, 8), (2, 8, 4))


def mod(x, y):
    return x % y if isinstance(x, int) else lax.rem(x, y)


def kernel(a_ref, g_ref, out_ref, at, gb, stg, own, ag, s0s, r1s, r2s, r3s, r1r, r2r, r3r,
           s0_send, s0_recv, r1_send, r1_recv, r2_send, r2_recv, r3_send, r3_recv,
           ag1_recv, ag2_recv, ag3_recv, ag1_send, ag2_send, ag3_send, core_send, core_recv, out_sem, g_sem, a_sem):
    _, mats, tokens, d = a_ref.shape
    per = g_ref.shape[3] // COLS
    units = mats * per
    chunks = tokens // CHUNK
    half, q1, q2, q3 = d // 2, d // 4, d // 8, d // 16
    f32, bf16 = jnp.float32, jnp.bfloat16

    me = lax.axis_index("dp")
    bit = {k: mod(me // k, 2) for k in (8, 4, 2, 1)}
    peer = {k: me + k - 2 * k * bit[k] for k in (8, 4, 2, 1)}
    c = bit[1]

    barrier = pltpu.get_barrier_semaphore()
    for k in (8, 4, 2, 1):
        pl.semaphore_signal(barrier, inc=1, device_id={"dp": peer[k]}, device_id_type=pl.DeviceIdType.MESH)
    pl.semaphore_wait(barrier, 4)

    class Unit:
        def __init__(self, s, i, lag):
            back, self.r = divmod(i - lag, TURN)
            self.w = TURN * s + (i - lag)
            self.s = s + back
            self.b = [bit[k] for k in ORDERS[self.r]]
            self.p = [peer[k] for k in ORDERS[self.r]]

        def slot(self, size):
            return self.r if size == TURN else TURN * mod(self.s + 8, size // TURN) + self.r

        def place(self):
            return self.s // (per // TURN), TURN * mod(self.s + 8 * per, per // TURN) + self.r

    def rows(start, size):
        return pl.ds(pl.multiple_of(start, 16), size)

    def remote(src, dst, send, recv, to):
        return pltpu.make_async_remote_copy(src_ref=src, dst_ref=dst, send_sem=send, recv_sem=recv,
                                            device_id={"dp": to}, device_id_type=pl.DeviceIdType.MESH)

    def load_g(u):
        n, j = u.place()
        slot = mod(u.w, 2)
        return pltpu.make_async_copy(
            g_ref.at[0, n, :, pl.ds(pl.multiple_of(j * COLS, COLS), COLS)], gb.at[slot], g_sem.at[slot])

    def load_a(n, i):
        slot = mod(i, 2)
        return pltpu.make_async_copy(
            a_ref.at[0, n, pl.ds(pl.multiple_of(i * CHUNK, CHUNK), CHUNK), :], stg.at[slot], a_sem.at[slot])

    def transpose(n, i):
        at[mod(n, 2), :, pl.ds(pl.multiple_of(i * CHUNK, CHUNK), CHUNK)] = stg[mod(i, 2)].T

    def dot(u, row):
        return jnp.dot(
            at[mod(u.place()[0], 2), rows(row, half), :], gb[mod(u.w, 2)], preferred_element_type=f32)

    def s0(u):
        k, m = u.slot(TURN), u.slot(LAND)
        return remote(s0s.at[k], ag.at[u.w], s0_send.at[k], s0_recv.at[m], peer[1])

    def r1(u):
        m, l = u.slot(RING), u.slot(LAND)
        return remote(r1s.at[m], r1r.at[l], r1_send.at[m], r1_recv.at[l], u.p[0])

    def r2(u):
        m, l = u.slot(RING), u.slot(LAND)
        return remote(r2s.at[m], r2r.at[l], r2_send.at[m], r2_recv.at[l], u.p[1])

    def r3(u):
        m, l = u.slot(RING), u.slot(LAND)
        return remote(r3s.at[m], r3r.at[l], r3_send.at[m], r3_recv.at[l], u.p[2])

    def g1(u):
        part = ag.at[u.w, rows(u.b[0] * q1 + u.b[1] * q2 + u.b[2] * q3, q3)]
        return remote(part, part, ag1_send, ag1_recv.at[u.w], u.p[2])

    def g2(u):
        part = ag.at[u.w, rows(u.b[0] * q1 + u.b[1] * q2, q2)]
        return remote(part, part, ag2_send, ag2_recv.at[u.w], u.p[1])

    def g3(u):
        part = ag.at[u.w, rows(u.b[0] * q1, q1)]
        return remote(part, part, ag3_send, ag3_recv.at[u.w], u.p[0])

    def finish(u):
        n, j = u.place()
        to = out_ref.at[n, rows(c * half, half), pl.ds(pl.multiple_of(j * COLS, COLS), COLS)]
        remote(ag.at[u.w], to, core_send, core_recv, peer[1]).start()
        pltpu.make_async_copy(ag.at[u.w], to, out_sem).start()

    def pieces(size, f):
        for i in range(size // PIECE):
            f(i * PIECE)

    def add(u, base, size, got, bit, send):
        k = u.slot(HELD)
        give, keep = (1 - bit) * size, bit * size

        def piece(off):
            send[rows(off, PIECE)] = (
                own[k, rows(base + give + off, PIECE)] + got[rows(give + off, PIECE)].astype(f32)).astype(bf16)
            kept = rows(base + keep + off, PIECE)
            own[k, kept] = own[k, kept] + got[rows(keep + off, PIECE)].astype(f32)

        pieces(size, piece)

    def add1(u):
        add(u, 0, q1, ag.at[u.w], u.b[0], r1s.at[u.slot(RING)])

    def add2(u):
        add(u, u.b[0] * q1, q2, r1r.at[u.slot(LAND)], u.b[1], r2s.at[u.slot(RING)])

    def add3(u):
        add(u, u.b[0] * q1 + u.b[1] * q2, q3, r2r.at[u.slot(LAND)], u.b[2], r3s.at[u.slot(RING)])

    def add4(u):
        k, m = u.slot(HELD), u.slot(LAND)
        base = u.b[0] * q1 + u.b[1] * q2 + u.b[2] * q3

        def piece(off):
            kept = rows(base + off, PIECE)
            ag[u.w, kept] = (own[k, kept] + r3r[m, rows(off, PIECE)].astype(f32)).astype(bf16)

        pieces(q3, piece)

    def gather1(u):
        g1(u).start()

    def gather2(u):
        g1(u).wait_recv()
        g2(u).start()

    def gather3(u):
        g2(u).wait_recv()
        g3(u).start()

    def gather4(u):
        g3(u).wait_recv()
        finish(u)

    def step(s, i, guard):
        t = TURN * s + i

        def do(lag, f):
            def run():
                f(Unit(s, i, lag))

            if guard:
                pl.when(jnp.logical_and(t >= lag, t - lag < units))(run)
            else:
                run()

        u = Unit(s, i, 0)
        n, j = u.place()
        more = n + 1 < mats

        @pl.when(t + 1 < units)
        def _():
            load_g(Unit(s, i, -1)).start()

        if i == 0:
            @pl.when(jnp.logical_and(more, j == 0))
            def _():
                load_a(n + 1, 0).start()

        @pl.when(jnp.logical_and(more, j + 1 < chunks))
        def _():
            load_a(n + 1, j + 1).start()

        @pl.when(jnp.logical_and(more, j < chunks))
        def _():
            load_a(n + 1, j).wait()
            transpose(n + 1, j)

        do(TURN, lambda u: s0(u).wait_send())
        load_g(u).wait()

        s0s[u.slot(TURN)] = dot(u, (1 - c) * half).astype(bf16)
        own[u.slot(HELD)] = dot(u, c * half)
        s0(u).start()

        def halve(lag, before, add, copy):
            do(lag, lambda u: before(u).wait_recv())
            do(lag + RING, lambda u: copy(u).wait_send())
            do(lag, add)
            do(lag, lambda u: copy(u).start())

        halve(E1, s0, add1, r1)
        halve(E2, r1, add2, r2)
        halve(E3, r2, add3, r3)
        do(E4, lambda u: r3(u).wait_recv())
        do(E4, add4)
        do(G1, gather1)
        do(G1 + LAG, gather2)
        do(G1 + 2 * LAG, gather3)
        do(G1 + 3 * LAG, gather4)

    def loop(lo, hi, guard):
        def body(s, _):
            for i in range(TURN):
                step(s, i, guard)
            return 0

        lax.fori_loop(lo, hi, body, 0)

    load_g(Unit(0, 0, 0)).start()
    load_a(0, 0).start()

    def first(i, _):
        @pl.when(i + 1 < chunks)
        def _():
            load_a(0, i + 1).start()

        load_a(0, i).wait()
        transpose(0, i)
        return 0

    lax.fori_loop(0, chunks, first, 0)

    deep = G1 + 3 * LAG
    turns = units // TURN
    full = -(-max(deep, E3 + RING) // TURN)
    loop(0, full, True)
    loop(full, turns, False)

    def last(lag):
        return units - lag

    at_stage = [last(lag) for lag in (E1, E2, E3, E4, G1, G1 + LAG, G1 + 2 * LAG, G1 + 3 * LAG)]
    ahead = units
    while at_stage[-1] < units:
        todo = []
        for lo in at_stage:
            todo.append([Unit(w // TURN, w % TURN, 0) for w in range(lo, ahead)])
            ahead = lo
        for u in todo[0]:
            s0(u).wait_recv()
            r1(Unit(u.s - RING // TURN, u.r, 0)).wait_send()
            add1(u)
            r1(u).start()
        for u in todo[1]:
            r1(u).wait_recv()
            r2(Unit(u.s - RING // TURN, u.r, 0)).wait_send()
            add2(u)
            r2(u).start()
        for u in todo[2]:
            r2(u).wait_recv()
            r3(Unit(u.s - RING // TURN, u.r, 0)).wait_send()
            add3(u)
            r3(u).start()
        for u in todo[3]:
            r3(u).wait_recv()
            add4(u)
        for u in todo[4] + todo[3]:
            gather1(u)
        for u in todo[5]:
            gather2(u)
        for u in todo[6]:
            gather3(u)
        for u in todo[7]:
            gather4(u)
        at_stage = [units] + at_stage[:3] + [at_stage[2]] + at_stage[4:7]
        ahead = units
    for u in [Unit(w // TURN, w % TURN, 0) for w in range(units - RING, units)]:
        r1(u).wait_send()
        r2(u).wait_send()
        r3(u).wait_send()

    for i in range(TURN):
        s0(Unit(turns - 1, i, 0)).wait_send()

    def all_of(size, sem):
        whole = ag.at[pl.ds(0, units * size // half)]
        pltpu.make_async_copy(whole, whole, sem).wait()

    all_of(q3, ag1_send)
    all_of(q2, ag2_send)
    all_of(q1, ag3_send)
    all_of(half, core_send)
    all_of(half, core_recv)
    all_of(half, out_sem)


def solution(mesh):
    def step(a, g):
        _, mats, tokens, d = a.shape
        ff = g.shape[3]
        units = mats * ff // COLS
        half = d // 2
        bf16 = jnp.bfloat16
        dma = pltpu.SemaphoreType.DMA
        return pl.pallas_call(
            kernel,
            out_shape=jax.ShapeDtypeStruct((mats, d, ff), bf16),
            in_specs=[pl.BlockSpec(memory_space=pl.ANY)] * 2,
            out_specs=pl.BlockSpec(memory_space=pl.ANY),
            scratch_shapes=[
                pltpu.VMEM((2, d, tokens), bf16),
                pltpu.VMEM((2, tokens, COLS), bf16),
                pltpu.VMEM((2, CHUNK, d), bf16),
                pltpu.VMEM((HELD, half, COLS), jnp.float32),
                pltpu.VMEM((units, half, COLS), bf16),
                pltpu.VMEM((3, half, COLS), bf16),
                pltpu.VMEM((RING, half // 2, COLS), bf16),
                pltpu.VMEM((RING, half // 4, COLS), bf16),
                pltpu.VMEM((RING, half // 8, COLS), bf16),
                pltpu.VMEM((LAND, half // 2, COLS), bf16),
                pltpu.VMEM((LAND, half // 4, COLS), bf16),
                pltpu.VMEM((LAND, half // 8, COLS), bf16),
                dma((TURN,)), dma((LAND,)), dma((RING,)), dma((LAND,)), dma((RING,)), dma((LAND,)), dma((RING,)), dma((LAND,)),
                dma((units,)), dma((units,)), dma((units,)), dma, dma, dma, dma, dma, dma, dma((2,)), dma((2,)),
            ],
            compiler_params=pltpu.CompilerParams(
                collective_id=0, has_side_effects=True, vmem_limit_bytes=64 * 1024 * 1024 - 65536),
            name="grads",
        )(a, g)

    return jax.shard_map(step, mesh=mesh, in_specs=(P(("rep", "dp")),) * 2, out_specs=P("rep"), check_vma=False)
```
